32 devices in a mesh: grp: 2 (over core), dom: 16 (over z, y, x).
Axes of the slice: x: 2, y: 2, z: 4, core: 2. Of those that a mesh axis runs over, the one named last changes fastest.
Arguments:
- node_latent: bfloat16 [32768, 128], P(('grp', 'dom')), may hold values from -6 to 6
- edge_latent: bfloat16 [196608, 128], P(('grp', 'dom')), may hold values from -6 to 6
- mig_send: int32 [32, 256], P(('grp', 'dom')), may hold values from 0 to 1024, as said below
- mig_recv: int32 [32768], P(('grp', 'dom')), may hold values from 0 to 1279, as said below
- halo_send: int32 [32, 128], P(('grp', 'dom')), may hold values from 0 to 1024, as said below
- cross_send: int32 [32, 32], P(('grp', 'dom')), may hold values from 0 to 1024, as said below
- senders: int32 [196608], P(('grp', 'dom')), may hold values from 0 to 1183, as said below
- receivers: int32 [196608], P(('grp', 'dom')), may hold values from 0 to 1023
- edge_live: int32 [196608], P(('grp', 'dom')), may hold values from 0 to 1, as said below
- edge_w1: bfloat16 [384, 128], replicated, may hold values from -0.3125 to 0.3125
- edge_b1: float32 [128], replicated, may hold values from -2 to 2
- edge_w2: bfloat16 [128, 128], replicated, may hold values from -0.5 to 0.5
- edge_b2: float32 [128], replicated, may hold values from -2 to 2
- edge_gain: float32 [128], replicated, may hold values from 0.25 to 1.75
- edge_bias: float32 [128], replicated, may hold values from -2 to 2
- node_w1: bfloat16 [256, 128], replicated, may hold values from -0.375 to 0.375
- node_b1: float32 [128], replicated, may hold values from -2 to 2
- node_w2: bfloat16 [128, 128], replicated, may hold values from -0.5 to 0.5
- node_b2: float32 [128], replicated, may hold values from -2 to 2
- node_gain: float32 [128], replicated, may hold values from 0.25 to 1.75
- node_bias: float32 [128], replicated, may hold values from -2 to 2
Outputs:
- node_out: bfloat16 [32768, 128], P(('grp', 'dom'))
- edge_out: bfloat16 [196608, 128], P(('grp', 'dom'))
The draws below stay inside these ranges and needn't reach their ends.
Inputs may be any that keep to these rules, and one draw needn't show every extreme that they name: `mig_send`: per partition, slot k * 64 + c names an old local row moving to the partition at distance o_k, or 1024 for an empty slot; live slots of one distance come first, every old row is named at most once, and a partition sends to a partition exactly as many rows as it receives from it. Where the peer exists, 32 or more slots of a distance are live; slots toward missing partitions are empty; in every draw some partition of each region fills all its slots both ways. `mig_recv`: for each partition, 1024 distinct entries of its source table: old rows it did not send and live arrived slots, each exactly once. `halo_send`: slot k * 32 + c names a new local row sent to the partition at distance o_k, or 1024 if empty; live slots come first, rows are distinct within a partition; where the peer exists 32 // 2 or more are live, and some partition of each region fills all slots whose peer exists. `cross_send`: new local rows sent to the same partition of the other region, or 1024 if empty; live slots come first, 16 or more live, distinct from that partition's halo_send rows; some partition of each region fills all. `senders`: each entry names a new local row (below 1024) or a live halo or cross slot of the extended table. `edge_live`: within a partition, the live edge slots are a prefix of at least 3072 slots; some partition is fully live in every draw.
All inputs are finite; a program needn't handle non-finite values.
Results may differ from the reference program's by a relative error of at most 0.0075.
Values may be sent and summed in bfloat16 or wider, within the bound.
No kernel may reach another device: no remote copies, remote signals or barrier semaphores. Data moves between devices by JAX's collectives and lax.ppermute only.
A program may use at most 64 MiB of HBM per device.

```python
import jax
import jax.numpy as jnp
from jax import lax

L = 128
R = 2
CAP = 64
HCAP = 32
XCAP = 32
TILE = 128
NODES_DEV = 1024
ETILES = 48
NODES = 32768
EDGES = 196608
N_GRP = 2
N_DOM = 16


def offset_list_drawn():
    return [number - R if number < R else number - R + 1 for number in range(2 * R)]


def move_counts(counts, shift_by):
    domain = jnp.arange(N_DOM, dtype=jnp.int32) - shift_by
    inside = (domain >= 0) & (domain < N_DOM)
    return jnp.where(inside[None, :], counts[:, jnp.clip(domain, 0, N_DOM - 1)], 0)


def distinct_order(key, length):
    scores = jax.random.randint(key, (N_GRP, N_DOM, length), 0, 2 ** 14) * 32768 + jnp.arange(length, dtype=jnp.int32)
    return jnp.argsort(scores, axis=-1).astype(jnp.int32)


def layout_plan(key):
    groups = N_GRP
    parts = N_DOM
    distances = 2 * R
    shifts = offset_list_drawn()
    domain = jnp.arange(parts, dtype=jnp.int32)
    centre = jax.random.randint(jax.random.fold_in(key, 11), (groups,), R, parts - R)
    flows = jax.random.randint(jax.random.fold_in(key, 12), (groups, parts, R), CAP // 2, CAP + 1)
    reach = jnp.arange(1, R + 1, dtype=jnp.int32)
    touches = (domain[None, :, None] == centre[:, None, None]) | (domain[None, :, None] + reach[None, None, :] == centre[:, None, None])
    flows = jnp.where(touches, CAP, flows)
    flows = jnp.where(domain[None, :, None] + reach[None, None, :] < parts, flows, 0)
    columns = []
    for shift in shifts:
        if shift > 0:
            columns.append(flows[:, :, shift - 1])
        else:
            columns.append(move_counts(flows[:, :, -shift - 1], -shift))
    counts = jnp.stack(columns, axis=2)
    arrivals = jnp.stack([move_counts(counts[:, :, place], shift) for place, shift in enumerate(shifts)], axis=2)
    order = distinct_order(jax.random.fold_in(key, 13), NODES_DEV)
    starts = jnp.cumsum(counts, axis=2) - counts
    outgoing = jnp.sum(counts, axis=2)
    slot_ids = jnp.arange(CAP, dtype=jnp.int32)
    positions = jnp.minimum(starts[..., None] + slot_ids, NODES_DEV - 1).reshape(groups, parts, distances * CAP)
    chosen = jnp.take_along_axis(order, positions, axis=2).reshape(groups, parts, distances, CAP)
    mig_send = jnp.where(slot_ids < counts[..., None], chosen, NODES_DEV).reshape(groups * parts, distances * CAP)
    ranks = jnp.argsort(order, axis=-1).astype(jnp.int32)
    kept = ranks >= outgoing[..., None]
    landed = (slot_ids < arrivals[..., None]).reshape(groups, parts, distances * CAP)
    usable = jnp.concatenate([kept, landed], axis=2).astype(jnp.int32)
    table_len = NODES_DEV + distances * CAP
    scores = (1 - usable) * 2 ** 30 + jax.random.randint(jax.random.fold_in(key, 14), (groups, parts, table_len), 0, 2 ** 14) * 32768 + jnp.arange(table_len, dtype=jnp.int32)
    mig_recv = jnp.argsort(scores, axis=-1).astype(jnp.int32)[..., :NODES_DEV].reshape(-1)
    halo_centre = jax.random.randint(jax.random.fold_in(key, 15), (groups,), 0, parts)
    halo_counts = jax.random.randint(jax.random.fold_in(key, 16), (groups, parts, distances), HCAP // 2, HCAP + 1)
    halo_counts = jnp.where(domain[None, :, None] == halo_centre[:, None, None], HCAP, halo_counts)
    shift_arr = jnp.array(shifts, dtype=jnp.int32)
    target = domain[None, :, None] + shift_arr[None, None, :]
    halo_counts = jnp.where((target >= 0) & (target < parts), halo_counts, 0)
    second = distinct_order(jax.random.fold_in(key, 17), NODES_DEV)
    halo_ids = jnp.arange(HCAP, dtype=jnp.int32)
    halo_rows = second[..., :distances * HCAP].reshape(groups, parts, distances, HCAP)
    halo_send = jnp.where(halo_ids < halo_counts[..., None], halo_rows, NODES_DEV).reshape(groups * parts, distances * HCAP)
    cross_counts = jax.random.randint(jax.random.fold_in(key, 18), (groups, parts), XCAP // 2, XCAP + 1)
    cross_counts = jnp.where(domain[None, :] == halo_centre[:, None], XCAP, cross_counts)
    cross_ids = jnp.arange(XCAP, dtype=jnp.int32)
    cross_rows = second[..., distances * HCAP:distances * HCAP + XCAP]
    cross_send = jnp.where(cross_ids < cross_counts[..., None], cross_rows, NODES_DEV).reshape(groups * parts, XCAP)
    halo_arrivals = jnp.stack([move_counts(halo_counts[:, :, place], shift) for place, shift in enumerate(shifts)], axis=2)
    cross_arrivals = jnp.flip(cross_counts, axis=0)
    remote_live = jnp.concatenate([(halo_ids < halo_arrivals[..., None]).reshape(groups, parts, distances * HCAP), cross_ids < cross_arrivals[..., None]], axis=2).astype(jnp.int32)
    return (mig_send, mig_recv, halo_send, cross_send, remote_live)


def draw_mig_send(key, part):
    return layout_plan(key)[0]


def draw_mig_recv(key, part):
    return layout_plan(key)[1]


def draw_halo_send(key, part):
    return layout_plan(key)[2]


def draw_cross_send(key, part):
    return layout_plan(key)[3]


def draw_senders(key, part):
    remote_live = layout_plan(key)[4]
    remote_len = remote_live.shape[2]
    edges_dev = ETILES * TILE
    scores = (1 - remote_live) * 65536 + jnp.arange(remote_len, dtype=jnp.int32)
    remote_order = jnp.argsort(scores, axis=-1).astype(jnp.int32)
    live_total = jnp.sum(remote_live, axis=2)
    picks = jax.random.randint(jax.random.fold_in(key, 21), (N_GRP, N_DOM, edges_dev), 0, 2 ** 20) % live_total[..., None]
    remote = NODES_DEV + jnp.take_along_axis(remote_order, picks, axis=2)
    local = jax.random.randint(jax.random.fold_in(key, 22), (N_GRP, N_DOM, edges_dev), 0, NODES_DEV)
    faraway = jax.random.randint(jax.random.fold_in(key, 23), (N_GRP, N_DOM, edges_dev), 0, 10) < 3
    return jnp.where(faraway, remote, local).astype(jnp.int32).reshape(-1)


def draw_edge_live(key, part):
    edges_dev = ETILES * TILE
    counts = jax.random.randint(jax.random.fold_in(key, 31), (N_GRP * N_DOM,), edges_dev // 2, edges_dev + 1)
    fullest = jax.random.randint(jax.random.fold_in(key, 32), (), 0, N_GRP * N_DOM)
    counts = jnp.where(jnp.arange(N_GRP * N_DOM, dtype=jnp.int32) == fullest, edges_dev, counts)
    slots = jnp.arange(edges_dev, dtype=jnp.int32)
    return (slots[None, :] < counts[:, None]).astype(jnp.int32).reshape(-1)


def touch_ends(entries, key, smallest, largest):
    dims = entries.shape
    spot = [jax.random.randint(jax.random.fold_in(key, axis), (), 0, dims[axis]) for axis in range(len(dims))]
    entries = entries.at[tuple(spot)].set(smallest)
    longest = dims.index(max(dims))
    spot[longest] = (spot[longest] + 1) % dims[longest]
    return entries.at[tuple(spot)].set(largest)


def block_scale(own_key, dims, cuts, least, largest):
    loudness = 1.0
    for dim, shards_of in cuts:
        draws = jax.random.uniform(jax.random.fold_in(jax.random.fold_in(own_key, 6), dim), (shards_of,), jnp.float32, least / len(cuts), largest / len(cuts))
        loudness = loudness * jnp.repeat(jnp.exp(draws), dims[dim] // shards_of).reshape((-1,) + (1,) * (len(dims) - 1 - dim))
    return loudness


def centred(own_key, shape, deviation, bound, split=(), kind=jnp.bfloat16):
    loudness = block_scale(own_key, shape, split, -0.22, 0.18) if split else 1.0
    drawn = jax.random.normal(own_key, shape, jnp.float32) * deviation * loudness
    return jnp.minimum(jnp.maximum(drawn, -bound), bound).astype(kind)


def setup_inputs(seed: int = 0) -> dict:
    streams_of = jax.random.split(jax.random.key(seed), 22)
    return {
        "node_latent": centred(streams_of[0], (NODES, L), 1.0, 6.0, ((0, 32),)),
        "edge_latent": centred(streams_of[1], (EDGES, L), 1.0, 6.0, ((0, 32),)),
        "mig_send": draw_mig_send(jax.random.fold_in(streams_of[21], 71), 0),
        "mig_recv": draw_mig_recv(jax.random.fold_in(streams_of[21], 71), 0),
        "halo_send": draw_halo_send(jax.random.fold_in(streams_of[21], 71), 0),
        "cross_send": draw_cross_send(jax.random.fold_in(streams_of[21], 71), 0),
        "senders": draw_senders(jax.random.fold_in(streams_of[21], 71), 0),
        "receivers": touch_ends(jax.random.randint(streams_of[7], (EDGES,), 0, NODES_DEV), jax.random.fold_in(streams_of[7], 1), 0, NODES_DEV - 1).astype(jnp.int32),
        "edge_live": draw_edge_live(jax.random.fold_in(streams_of[21], 71), 0),
        "edge_w1": centred(streams_of[9], (3 * L, L), (3 * L) ** -0.5, 0.3125),
        "edge_b1": centred(streams_of[10], (L,), 0.3, 2.0, (), jnp.float32),
        "edge_w2": centred(streams_of[11], (L, L), L ** -0.5, 0.5),
        "edge_b2": centred(streams_of[12], (L,), 0.3, 2.0, (), jnp.float32),
        "edge_gain": jnp.clip(1.0 + 0.15 * jax.random.normal(streams_of[13], (L,), jnp.float32), 0.25, 1.75),
        "edge_bias": centred(streams_of[14], (L,), 0.3, 2.0, (), jnp.float32),
        "node_w1": centred(streams_of[15], (2 * L, L), (2 * L) ** -0.5, 0.375),
        "node_b1": centred(streams_of[16], (L,), 0.3, 2.0, (), jnp.float32),
        "node_w2": centred(streams_of[17], (L, L), L ** -0.5, 0.5),
        "node_b2": centred(streams_of[18], (L,), 0.3, 2.0, (), jnp.float32),
        "node_gain": jnp.clip(1.0 + 0.15 * jax.random.normal(streams_of[19], (L,), jnp.float32), 0.25, 1.75),
        "node_bias": centred(streams_of[20], (L,), 0.3, 2.0, (), jnp.float32),
    }


EPSILON = 1e-05

def offset_list():
    return [number - R if number < R else number - R + 1 for number in range(2 * R)]

def layer_norm(values, scale_vec, offset_vec):
    center = values - lax.optimization_barrier(jnp.mean(values, axis=-1, keepdims=True))
    spread = lax.optimization_barrier(jnp.mean(center * center, axis=-1, keepdims=True))
    return center * lax.rsqrt(spread + EPSILON) * scale_vec + offset_vec

def select_rows(source_rows, wanted):
    padded = jnp.concatenate([source_rows, jnp.zeros((1, source_rows.shape[1]), source_rows.dtype)], axis=0)
    return padded[jnp.minimum(wanted, source_rows.shape[0]).astype(jnp.int32)]

def move_along(stacked, shift_by):
    domain = jnp.arange(N_DOM, dtype=jnp.int32) - shift_by
    inside = (domain >= 0) & (domain < N_DOM)
    moved = stacked[:, jnp.clip(domain, 0, N_DOM - 1)]
    inside = inside.reshape((1, N_DOM) + (1,) * (stacked.ndim - 2))
    return jnp.where(inside, moved, jnp.zeros((), stacked.dtype))

def deliver(outgoing):
    return jnp.stack([move_along(outgoing[:, :, position], shift) for position, shift in enumerate(offset_list())], axis=2)

def reference(node_latent, edge_latent, mig_send, mig_recv, halo_send, cross_send, senders, receivers, edge_live, edge_w1, edge_b1, edge_w2, edge_b2, edge_gain, edge_bias, node_w1, node_b1, node_w2, node_b2, node_gain, node_bias):
    latent = node_latent.shape[1]
    groups = N_GRP
    parts = N_DOM
    per_device = jax.vmap(jax.vmap(select_rows))
    old_rows = node_latent.reshape(groups, parts, NODES_DEV, latent)
    leaving = per_device(old_rows, mig_send.reshape(groups, parts, 2 * R * CAP)).reshape(groups, parts, 2 * R, CAP, latent)
    arrived = deliver(leaving).reshape(groups, parts, 2 * R * CAP, latent)
    source_rows = jnp.concatenate([old_rows, arrived], axis=2)
    direct_take = jax.vmap(jax.vmap(lambda table_rows, wanted: table_rows[wanted]))
    fresh = direct_take(source_rows, mig_recv.reshape(groups, parts, NODES_DEV))
    halo_out = per_device(fresh, halo_send.reshape(groups, parts, 2 * R * HCAP)).reshape(groups, parts, 2 * R, HCAP, latent)
    halo_in = deliver(halo_out).reshape(groups, parts, 2 * R * HCAP, latent)
    cross_out = per_device(fresh, cross_send.reshape(groups, parts, XCAP))
    cross_in = jnp.flip(cross_out, axis=0)
    extended = jnp.concatenate([fresh, halo_in, cross_in], axis=2).reshape(groups * parts, -1, latent)
    fresh_flat = fresh.reshape(groups * parts, NODES_DEV, latent)
    edges_dev = ETILES * TILE
    wide = jnp.float32

    def device_layer(items):
        fresh_rows, extended_rows, edge_rows, sender_ids, receiver_ids, active = items
        sent_side = extended_rows[sender_ids]
        recv_side = fresh_rows[receiver_ids]
        joined = jnp.concatenate([edge_rows, sent_side, recv_side], axis=1).astype(wide)
        hidden = jnp.maximum(jnp.dot(joined, edge_w1.astype(wide)) + edge_b1, 0.0).astype(jnp.bfloat16)
        before = jnp.dot(hidden.astype(wide), edge_w2.astype(wide)) + edge_b2
        message = layer_norm(before, edge_gain, edge_bias).astype(jnp.bfloat16)
        kept = message.astype(wide) * active.astype(wide)[:, None]
        new_edges = (edge_rows.astype(wide) + kept).astype(jnp.bfloat16)
        inbound = jax.ops.segment_sum(kept, receiver_ids, num_segments=NODES_DEV).astype(jnp.bfloat16)
        node_in = jnp.concatenate([fresh_rows, inbound], axis=1).astype(wide)
        node_hidden = jnp.maximum(jnp.dot(node_in, node_w1.astype(wide)) + node_b1, 0.0).astype(jnp.bfloat16)
        node_before = jnp.dot(node_hidden.astype(wide), node_w2.astype(wide)) + node_b2
        new_nodes = (fresh_rows.astype(wide) + layer_norm(node_before, node_gain, node_bias)).astype(jnp.bfloat16)
        return (new_nodes, new_edges)
    new_nodes, new_edges = lax.map(device_layer, (fresh_flat, extended, edge_latent.reshape(groups * parts, edges_dev, latent), senders.reshape(groups * parts, edges_dev), receivers.reshape(groups * parts, edges_dev), edge_live.reshape(groups * parts, edges_dev)))
    return (new_nodes.reshape(-1, latent), new_edges.reshape(-1, latent))
```

```python
import functools

import jax
import jax.numpy as jnp
from jax import lax
from jax.experimental import pallas as pl
from jax.experimental.pallas import tpu as pltpu
from jax.sharding import PartitionSpec as P

R = 2
LANES = 128
EDGE_BLOCK = 1024
ANY = pl.BlockSpec(memory_space=pl.ANY)
EPSILON = 1e-05
BF16 = jnp.bfloat16
F32 = jnp.float32


def dot(a, b):
    return jnp.dot(a, b, preferred_element_type=F32)


def swapped(value, axis, partner_of):
    count = lax.axis_size(axis)
    pairs = []
    for i in range(count):
        j = partner_of(i)
        pairs.append((i, j if 0 <= j < count else i))
    return lax.ppermute(value, axis, pairs)


def lane_ids(tile, shift):
    ids = lax.broadcasted_iota(jnp.int32, (LANES, LANES), 1) + (tile * LANES - shift)
    return ids.astype(F32).astype(BF16)


def spread(columns, b):
    return jnp.broadcast_to(columns[:, b : b + 1], (columns.shape[0], LANES))


def marks_from(values, count, shift):
    one, zero = jnp.ones((), BF16), jnp.zeros((), BF16)
    values = values.astype(BF16)
    rows = values.shape[0]
    return jnp.concatenate(
        [jnp.where(values == lane_ids(t, shift)[:rows], one, zero) for t in range(count)], axis=1
    )


def split_index(rows, half):
    high = (rows >= half).astype(F32)
    low = rows.astype(F32) - high * half - half // 2
    return low.T, high.T


def lookup(low, high, b, table2):
    half = table2.shape[0]
    both = dot(marks_from(spread(low, b), half // LANES, half // 2), table2)
    return jnp.where(spread(high, b) > 0.5, both[:, LANES:], both[:, :LANES])


def side_by_side(table):
    half = table.shape[0] // 2
    return jnp.concatenate([table[:half], table[half:]], axis=1)


def twice(w):
    zero = jnp.zeros_like(w)
    return jnp.concatenate(
        [jnp.concatenate([w, zero], axis=1), jnp.concatenate([zero, w], axis=1)], axis=0
    )


def eight(row):
    return jnp.broadcast_to(row, (8, row.shape[1]))


def leave_kernel(node_hbm, send_hbm, near_ref, far_ref, node_ref, send_ref, sems):
    copies = [
        pltpu.make_async_copy(send_hbm, send_ref, sems.at[0]),
        pltpu.make_async_copy(node_hbm, node_ref, sems.at[1]),
    ]
    for copy in copies:
        copy.start()
    for copy in copies:
        copy.wait()
    table = side_by_side(node_ref[...])
    pieces = []
    for b in range(send_ref.shape[1] // LANES):
        low, high = split_index(eight(send_ref[:, b * LANES : (b + 1) * LANES]), table.shape[0])
        pieces.append(lookup(low, high, 0, table))
    rows = jnp.concatenate(pieces, axis=0).astype(BF16)
    quarter = rows.shape[0] // 4
    near_ref[...] = rows[quarter : 3 * quarter]
    far_ref[...] = jnp.concatenate([rows[:quarter], rows[3 * quarter :]], axis=0)


def own_kernel(
    edge_ref, w1_ref, b1_ref, send_ref, recv_ref, live_ref, mig_ref, halo_ref, cross_ref, _,
    own_ref, w1_copy, send_copy, recv_copy, live_copy, mig_copy, halo_copy, cross_copy,
):
    w1_copy[...] = w1_ref[...]
    send_copy[...] = send_ref[...]
    recv_copy[...] = recv_ref[...]
    live_copy[...] = live_ref[...]
    mig_copy[...] = mig_ref[...]
    halo_copy[...] = halo_ref[...]
    cross_copy[...] = cross_ref[...]
    wa = twice(w1_ref[:LANES, :])
    b1 = b1_ref[...]
    half = EDGE_BLOCK // 2

    def step(i, carry):
        at = pl.multiple_of(i * EDGE_BLOCK, EDGE_BLOCK)
        top, bottom = edge_ref[pl.ds(at, half), :], edge_ref[pl.ds(at + half, half), :]
        pair = dot(jnp.concatenate([top, bottom], axis=1), wa)
        own_ref[pl.ds(at, half), :] = pair[:, :LANES] + b1
        own_ref[pl.ds(at + half, half), :] = pair[:, LANES:] + b1
        return carry

    lax.fori_loop(0, edge_ref.shape[0] // EDGE_BLOCK, step, 0)


def target_kernel(recv_ref, node_ref, _, marks_ref, table_ref):
    table_ref[...] = side_by_side(node_ref[...])
    half = marks_ref.shape[0]
    one, zero = jnp.ones((), BF16), jnp.zeros((), BF16)
    ids = (lax.broadcasted_iota(jnp.int32, (half, LANES), 0) - half // 2).astype(F32).astype(BF16)
    recv = recv_ref[...]
    low = jnp.where(recv >= half, recv - half, recv) - half // 2
    low = low.astype(F32)
    for b in range(recv.shape[0]):
        row = jnp.broadcast_to(low[b : b + 1, :], (16, LANES)).astype(BF16)
        row = jnp.concatenate([row] * (half // 16), axis=0)
        marks_ref[:, b * LANES : (b + 1) * LANES] = jnp.where(ids == row, one, zero)


def fresh_kernel(
    table_ref, arrived_ref, recv_ref, halo_ref, cross_ref, fresh_ref, near_ref, far_ref, cross_out
):
    table = table_ref[...]
    n = 2 * table.shape[0]
    recv = recv_ref[...]
    low, high = split_index(recv, table.shape[0])
    moved = (recv - n).astype(F32).T
    arrived = arrived_ref[...]
    pieces = []
    for b in range(n // LANES):
        marks = marks_from(spread(moved, b), arrived.shape[0] // LANES, 0)
        pieces.append((lookup(low, high, b, table) + dot(marks, arrived)).astype(BF16))
    fresh = jnp.concatenate(pieces, axis=0)
    fresh_ref[...] = fresh
    table = side_by_side(fresh)
    low, high = split_index(eight(halo_ref[...]), table.shape[0])
    halo = lookup(low, high, 0, table).astype(BF16)
    quarter = halo.shape[0] // 4
    near_ref[...] = halo[quarter : 3 * quarter]
    far_ref[...] = jnp.concatenate([halo[:quarter], halo[3 * quarter :]], axis=0)
    low, high = split_index(eight(cross_ref[...]), table.shape[0])
    cross_out[...] = lookup(low, high, 0, table).astype(BF16)


def pre_kernel(before_ref, fresh_ref, index_ref, w_ref, _, out_ref, *, part):
    table = side_by_side(dot(fresh_ref[...], w_ref[part * LANES : (part + 1) * LANES, :]).astype(BF16))

    def step(i, carry):
        low, high = split_index(
            index_ref[pl.ds(pl.multiple_of(i * 8, 8), 8), :], table.shape[0]
        )
        for b in range(EDGE_BLOCK // LANES):
            at = pl.ds(pl.multiple_of(i * EDGE_BLOCK + b * LANES, LANES), LANES)
            out_ref[at, :] = before_ref[at, :] + lookup(low, high, b, table)
        return carry

    lax.fori_loop(0, out_ref.shape[0] // EDGE_BLOCK, step, 0)


def edge_kernel(
    pre_ref, edge_ref, fresh_ref, halo_ref, cross_ref, send_ref, recv_ref, live_ref, target_ref,
    w1_ref, w2_ref, b2_ref, gain_ref, bias_ref,
    nw1_ref, nb1_ref, nw2_ref, nb2_ref, ngain_ref, nbias_ref,
    node_out_ref, edge_out_ref,
    new_ref, acc_ref, sems,
):
    n = fresh_ref.shape[0]
    block = EDGE_BLOCK
    half = block // 2
    blocks = block // LANES
    nodes_half = n // 2

    r = lax.broadcasted_iota(jnp.int32, (2 * LANES, 2 * LANES), 0) // LANES
    c = lax.broadcasted_iota(jnp.int32, (2 * LANES, 2 * LANES), 1) // LANES
    averages = jnp.where(r == c, 1.0 / LANES, 0.0).astype(BF16)
    b2 = b2_ref[...]
    b2 = b2 - jnp.mean(b2, axis=-1, keepdims=True)
    b2 = jnp.concatenate([b2, b2], axis=1)
    remote_rows = jnp.concatenate([halo_ref[...], cross_ref[...]], axis=0)
    tx = dot(remote_rows, w1_ref[LANES : 2 * LANES, :]).astype(BF16)
    tx = jnp.concatenate([tx, jnp.zeros((2 * LANES - tx.shape[0], LANES), BF16)], axis=0)
    w2 = w2_ref[...].astype(F32)
    w2 = twice((w2 - jnp.mean(w2, axis=-1, keepdims=True)).astype(BF16))
    gain, bias = gain_ref[...], bias_ref[...]
    acc_ref[...] = jnp.zeros_like(acc_ref)

    def copy_out(i):
        at = pl.ds(pl.multiple_of(i * block, block), block)
        return pltpu.make_async_copy(new_ref.at[at, :], edge_out_ref.at[at, :], sems.at[i])

    def step(i, carry):
        rows8 = pl.ds(pl.multiple_of(i * 8, 8), 8)
        remote = (send_ref[rows8, :] - n).astype(F32).T
        high = (recv_ref[rows8, :] >= nodes_half).astype(F32).T
        live = live_ref[rows8, :].astype(F32).T
        hidden = []
        for b in range(blocks):
            at = pl.ds(pl.multiple_of(i * block + b * LANES, LANES), LANES)
            pre = pre_ref[at, :] + dot(marks_from(spread(remote, b), 2, 0), tx)
            hidden.append(jnp.maximum(pre, 0.0).astype(BF16))
        packed = []
        for b in range(blocks // 2):
            both = jnp.concatenate([hidden[b], hidden[b + blocks // 2]], axis=1)
            centre = dot(both, w2) + b2
            spreads = dot((centre * centre).astype(BF16), averages)
            normed = centre * lax.rsqrt(spreads + EPSILON)
            for k in range(2):
                bb = b + k * (blocks // 2)
                at = pl.ds(pl.multiple_of(i * block + bb * LANES, LANES), LANES)
                message = normed[:, k * LANES : (k + 1) * LANES] * gain + bias
                kept = message.astype(BF16).astype(F32) * spread(live, bb)
                new_ref[at, :] = (edge_ref[at, :].astype(F32) + kept).astype(BF16)
                upper = kept * spread(high, bb)
                packed.append((bb, jnp.concatenate([kept - upper, upper], axis=1).astype(BF16)))
        copy_out(i).start()
        packed = jnp.concatenate([p for _, p in sorted(packed, key=lambda p: p[0])], axis=0)
        marks = target_ref[:, pl.ds(pl.multiple_of(i * block, block), block)]
        acc_ref[...] += dot(marks, packed)
        return carry

    steps = pre_ref.shape[0] // block
    lax.fori_loop(0, steps, step, 0)
    fresh = fresh_ref[...]
    inbound = jnp.concatenate([acc_ref[:, :LANES], acc_ref[:, LANES:]], axis=0).astype(BF16)
    hidden_n = dot(jnp.concatenate([fresh, inbound], axis=1), nw1_ref[...]) + nb1_ref[...]
    hidden_n = jnp.maximum(hidden_n, 0.0).astype(BF16)
    nb2 = nb2_ref[...]
    nb2 = nb2 - jnp.mean(nb2, axis=-1, keepdims=True)
    nw2 = nw2_ref[...].astype(F32)
    nw2 = twice((nw2 - jnp.mean(nw2, axis=-1, keepdims=True)).astype(BF16))
    centre = dot(side_by_side(hidden_n), nw2) + jnp.concatenate([nb2, nb2], axis=1)
    spreads = dot((centre * centre).astype(BF16), averages)
    normed = centre * lax.rsqrt(spreads + EPSILON)
    for k in range(2):
        rows = slice(k * nodes_half, (k + 1) * nodes_half)
        update = normed[:, k * LANES : (k + 1) * LANES] * ngain_ref[...] + nbias_ref[...]
        node_out_ref[rows, :] = (fresh[rows].astype(F32) + update).astype(BF16)
    for i in range(steps):
        copy_out(i).wait()


def outward(near_partner, far, d):
    rows = far.shape[0] // 2
    even_pair = (d // 2) % 2 == 0
    plus = jnp.concatenate([far[rows:], near_partner[rows:]], axis=0)
    minus = jnp.concatenate([far[:rows], near_partner[:rows]], axis=0)
    outer = swapped(
        jnp.where(even_pair, minus, plus), "dom", lambda i: i - 2 if i % 4 < 2 else i + 2
    )
    inner = swapped(
        jnp.where(even_pair, plus, minus), "dom", lambda i: i + 2 if i % 4 < 2 else i - 2
    )
    return outer, inner


def inward(near_partner, outer, inner, d):
    rows = near_partner.shape[0] // 2
    odd = d % 2 == 1
    even_pair = (d // 2) % 2 == 0
    before = jnp.where(even_pair, outer, inner)
    after = jnp.where(even_pair, inner, outer)
    return jnp.concatenate(
        [
            after[:rows],
            jnp.where(odd, after[rows:], near_partner[:rows]),
            jnp.where(odd, near_partner[rows:], before[rows:]),
            before[:rows],
        ],
        axis=0,
    )


def call(kernel, name, out_shape, limit, flops=10**9, **kw):
    return pl.pallas_call(
        kernel,
        out_shape=out_shape,
        name=name,
        compiler_params=pltpu.CompilerParams(vmem_limit_bytes=limit << 20),
        cost_estimate=pl.CostEstimate(flops=flops, bytes_accessed=10**6, transcendentals=0),
        **kw,
    )


VM = pl.BlockSpec(memory_space=pltpu.VMEM)
HBM = pl.BlockSpec(memory_space=pltpu.MemorySpace.HBM)


def like(*arrays):
    return [jax.ShapeDtypeStruct(a.shape, a.dtype) for a in arrays]


def body(
    node_latent, edge_latent, mig_send, mig_recv, halo_send, cross_send, senders, receivers, edge_live,
    edge_w1, edge_b1, edge_w2, edge_b2, edge_gain, edge_bias,
    node_w1, node_b1, node_w2, node_b2, node_gain, node_bias,
):
    n, latent = node_latent.shape
    edges = edge_latent.shape[0]
    d = lax.axis_index("dom")
    move = mig_send.shape[1]
    halo = halo_send.shape[1]
    cross = cross_send.shape[1]
    shape = jax.ShapeDtypeStruct
    row = lambda v: v.reshape(1, latent)
    tiles = lambda v: v.reshape(-1, LANES)

    near, far = call(
        leave_kernel,
        "leave",
        [shape((move // 2, latent), BF16)] * 2,
        4,
        in_specs=[HBM] * 2,
        scratch_shapes=[
            pltpu.VMEM(node_latent.shape, BF16),
            pltpu.VMEM(mig_send.shape, jnp.int32),
            pltpu.SemaphoreType.DMA((2,)),
        ],
    )(node_latent, mig_send)
    partner = swapped(near, "dom", lambda i: i ^ 1)
    args = (
        edge_latent, edge_w1, row(edge_b1), tiles(senders), tiles(receivers), tiles(edge_live),
        tiles(mig_recv), halo_send, cross_send,
    )
    own, w1, send, recv, live, mig, halo_index, cross_index = call(
        own_kernel,
        "own",
        [shape((edges, latent), F32)] + like(args[1], *args[3:]),
        10,
        in_specs=[VM] * 9 + [ANY],
    )(*args, near)
    partner, own, recv = lax.optimization_barrier((partner, own, recv))
    outer, inner = outward(partner, far, d)
    targets, table = call(
        target_kernel,
        "targets",
        [shape((n // 2, edges), BF16), shape((n // 2, 2 * latent), BF16)],
        10,
        in_specs=[VM, VM, ANY],
    )(recv, node_latent, partner)
    outer, inner, targets, table = lax.optimization_barrier((outer, inner, targets, table))
    arrived = inward(partner, outer, inner, d)

    fresh, near, far, cross_out = call(
        fresh_kernel,
        "fresh",
        [shape((n, latent), BF16)] + [shape((halo // 2, latent), BF16)] * 2 + [shape((cross, latent), BF16)],
        8,
    )(table, arrived, mig, halo_index, cross_index)
    partner = swapped(near, "dom", lambda i: i ^ 1)
    cross_in = lax.ppermute(cross_out, "grp", [(i, i ^ 1) for i in range(lax.axis_size("grp"))])
    (pre,) = call(
        functools.partial(pre_kernel, part=2), "received", [shape((edges, latent), F32)], 10,
        in_specs=[VM] * 4 + [ANY],
    )(own, fresh, recv, w1, near)
    partner, pre = lax.optimization_barrier((partner, pre))
    outer, inner = outward(partner, far, d)
    (pre,) = call(
        functools.partial(pre_kernel, part=1), "sent", [shape((edges, latent), F32)], 10,
        in_specs=[VM] * 4 + [ANY],
    )(pre, fresh, send, w1, partner)
    outer, inner, cross_in, pre = lax.optimization_barrier((outer, inner, cross_in, pre))
    halo_in = inward(partner, outer, inner, d)
    node_out, edge_out = call(
        edge_kernel,
        "edges",
        [shape((n, latent), BF16), shape((edges, latent), BF16)],
        16,
        flops=10**10,
        out_specs=[VM, ANY],
        scratch_shapes=[
            pltpu.VMEM((edges, latent), BF16),
            pltpu.VMEM((n // 2, 2 * latent), F32),
            pltpu.SemaphoreType.DMA((edges // EDGE_BLOCK,)),
        ],
    )(
        pre, edge_latent, fresh, halo_in, cross_in, send, recv, live, targets,
        w1, edge_w2, row(edge_b2), row(edge_gain), row(edge_bias),
        node_w1, row(node_b1), node_w2, row(node_b2), row(node_gain), row(node_bias),
    )
    return node_out, edge_out


def solution(mesh):
    split, split1, copied = P(("grp", "dom"), None), P(("grp", "dom")), P()
    placed = (
        split, split, split, split1, split, split, split1, split1, split1,
    ) + (copied,) * 12
    return jax.shard_map(
        body, mesh=mesh, in_specs=placed, out_specs=(split, split), check_vma=False
    )
```

```python
import functools

import jax
import jax.numpy as jnp
from jax import lax
from jax.experimental import pallas as pl
from jax.experimental.pallas import tpu as pltpu
from jax.sharding import PartitionSpec as P


LANES = 128
EDGE_BLOCK = 1024
ANY = pl.BlockSpec(memory_space=pl.ANY)
EPSILON = 1e-05
BF16 = jnp.bfloat16
F32 = jnp.float32


def dot(a, b):
    return jnp.dot(a, b, preferred_element_type=F32)


def swapped(value, axis, partner_of):
    count = lax.axis_size(axis)
    pairs = []
    for i in range(count):
        j = partner_of(i)
        pairs.append((i, j if 0 <= j < count else i ^ 1))
    return lax.ppermute(value, axis, pairs)


def lane_ids(tile, shift):
    ids = lax.broadcasted_iota(jnp.int32, (LANES, LANES), 1) + (tile * LANES - shift)
    return ids.astype(F32).astype(BF16)


def spread(columns, b):
    return jnp.broadcast_to(columns[:, b : b + 1], (columns.shape[0], LANES))


def marks_from(values, count, shift):
    one, zero = jnp.ones((), BF16), jnp.zeros((), BF16)
    rows = values.shape[0]
    return jnp.concatenate(
        [jnp.where(values == lane_ids(t, shift)[:rows], one, zero) for t in range(count)], axis=1
    )


def split_index(rows, half):
    high = (rows >= half).astype(F32)
    low = rows.astype(F32) - high * half - half // 2
    return low.T.astype(BF16), high.T


def lookup(low, high, b, table2):
    half = table2.shape[0]
    both = dot(marks_from(spread(low, b), half // LANES, half // 2), table2)
    return jnp.where(spread(high, b) > 0.5, both[:, LANES:], both[:, :LANES])


def side_by_side(table):
    half = table.shape[0] // 2
    return jnp.concatenate([table[:half], table[half:]], axis=1)


def twice(w):
    zero = jnp.zeros_like(w)
    return jnp.concatenate(
        [jnp.concatenate([w, zero], axis=1), jnp.concatenate([zero, w], axis=1)], axis=0
    )


def eight(row):
    return jnp.broadcast_to(row, (8, row.shape[1]))


def first_kernel(out_ref):
    out_ref[...] = jnp.zeros_like(out_ref)


def leave_kernel(node_ref, send_ref, _, near_ref, far_ref):
    table = side_by_side(node_ref[...])
    pieces = []
    for b in range(send_ref.shape[1] // LANES):
        low, high = split_index(eight(send_ref[:, b * LANES : (b + 1) * LANES]), table.shape[0])
        pieces.append(lookup(low, high, 0, table))
    rows = jnp.concatenate(pieces, axis=0).astype(BF16)
    quarter = rows.shape[0] // 4
    near_ref[...] = rows[quarter : 3 * quarter]
    far_ref[...] = jnp.concatenate([rows[:quarter], rows[3 * quarter :]], axis=0)


def own_kernel(
    edge_ref, w1_ref, b1_ref, send_ref, recv_ref, live_ref, mig_ref, halo_ref, cross_ref, _,
    own_ref, w1_copy, send_copy, recv_copy, live_copy, mig_copy, halo_copy, cross_copy,
):
    w1_copy[...] = w1_ref[...]
    send_copy[...] = send_ref[...]
    recv_copy[...] = recv_ref[...]
    live_copy[...] = live_ref[...]
    mig_copy[...] = mig_ref[...]
    halo_copy[...] = halo_ref[...]
    cross_copy[...] = cross_ref[...]
    wa = twice(w1_ref[:LANES, :])
    b1 = b1_ref[...]
    half = EDGE_BLOCK // 2

    def step(i, carry):
        at = pl.multiple_of(i * EDGE_BLOCK, EDGE_BLOCK)
        top, bottom = edge_ref[pl.ds(at, half), :], edge_ref[pl.ds(at + half, half), :]
        pair = dot(jnp.concatenate([top, bottom], axis=1), wa)
        own_ref[pl.ds(at, half), :] = pair[:, :LANES] + b1
        own_ref[pl.ds(at + half, half), :] = pair[:, LANES:] + b1
        return carry

    lax.fori_loop(0, edge_ref.shape[0] // EDGE_BLOCK, step, 0)


def target_kernel(recv_ref, _, marks_ref):
    half = marks_ref.shape[0]
    one, zero = jnp.ones((), BF16), jnp.zeros((), BF16)
    ids = (lax.broadcasted_iota(jnp.int32, (half, LANES), 0) - half // 2).astype(F32).astype(BF16)
    recv = recv_ref[...]
    low = jnp.where(recv >= half, recv - half, recv) - half // 2
    low = low.astype(F32)
    for b in range(recv.shape[0]):
        row = jnp.broadcast_to(low[b : b + 1, :], (16, LANES)).astype(BF16)
        row = jnp.concatenate([row] * (half // 16), axis=0)
        marks_ref[:, b * LANES : (b + 1) * LANES] = jnp.where(ids == row, one, zero)


def fresh_kernel(
    node_ref, arrived_ref, recv_ref, halo_ref, cross_ref, fresh_ref, near_ref, far_ref, cross_out
):
    table = side_by_side(node_ref[...])
    n = 2 * table.shape[0]
    recv = recv_ref[...]
    low, high = split_index(recv, table.shape[0])
    moved = (recv - n).astype(F32).T.astype(BF16)
    arrived = arrived_ref[...]
    pieces = []
    for b in range(n // LANES):
        marks = marks_from(spread(moved, b), arrived.shape[0] // LANES, 0)
        pieces.append((lookup(low, high, b, table) + dot(marks, arrived)).astype(BF16))
    fresh = jnp.concatenate(pieces, axis=0)
    fresh_ref[...] = fresh
    table = side_by_side(fresh)
    low, high = split_index(eight(halo_ref[...]), table.shape[0])
    halo = lookup(low, high, 0, table).astype(BF16)
    quarter = halo.shape[0] // 4
    near_ref[...] = halo[quarter : 3 * quarter]
    far_ref[...] = jnp.concatenate([halo[:quarter], halo[3 * quarter :]], axis=0)
    low, high = split_index(eight(cross_ref[...]), table.shape[0])
    cross_out[...] = lookup(low, high, 0, table).astype(BF16)


def pre_kernel(before_ref, fresh_ref, index_ref, w_ref, _, out_ref, *, part):
    table = side_by_side(dot(fresh_ref[...], w_ref[part * LANES : (part + 1) * LANES, :]).astype(BF16))
    for i in range(out_ref.shape[0] // EDGE_BLOCK):
        low, high = split_index(index_ref[i * 8 : (i + 1) * 8, :], table.shape[0])
        for b in range(EDGE_BLOCK // LANES):
            at = slice(i * EDGE_BLOCK + b * LANES, i * EDGE_BLOCK + (b + 1) * LANES)
            out_ref[at, :] = before_ref[at, :] + lookup(low, high, b, table)


def edge_kernel(
    pre_ref, edge_ref, fresh_ref, halo_ref, cross_ref, send_ref, recv_ref, live_ref, target_ref,
    w1_ref, w2_ref, b2_ref, gain_ref, bias_ref,
    nw1_ref, nb1_ref, nw2_ref, nb2_ref, ngain_ref, nbias_ref,
    node_out_ref, edge_out_ref,
    new_ref, acc_ref, hidden_ref, packed_ref, node_ref, sems, node_sems,
):
    n = fresh_ref.shape[0]
    nodes_half = n // 2
    block = EDGE_BLOCK
    quarters = block // (2 * LANES)

    r = lax.broadcasted_iota(jnp.int32, (2 * LANES, 2 * LANES), 0) // LANES
    c = lax.broadcasted_iota(jnp.int32, (2 * LANES, 2 * LANES), 1) // LANES
    averages = jnp.where(r == c, 1.0 / LANES, 0.0).astype(BF16)
    b2 = b2_ref[...]
    b2 = b2 - jnp.mean(b2, axis=-1, keepdims=True)
    b2 = jnp.concatenate([b2, b2], axis=1)
    remote_rows = jnp.concatenate([halo_ref[...], cross_ref[...]], axis=0)
    tx = dot(remote_rows, w1_ref[LANES : 2 * LANES, :]).astype(BF16)
    tx = jnp.concatenate([tx, jnp.zeros((2 * LANES - tx.shape[0], LANES), BF16)], axis=0)
    w2 = w2_ref[...].astype(F32)
    w2 = twice((w2 - jnp.mean(w2, axis=-1, keepdims=True)).astype(BF16))
    gain, bias = gain_ref[...], bias_ref[...]
    acc_ref[...] = jnp.zeros_like(acc_ref)

    def rows_of(j, offset, size):
        return pl.ds(pl.multiple_of(j * block + offset, LANES), size)

    def tile_of(ref, j):
        return ref[pl.ds(pl.multiple_of(j * 8, 8), 8), :]

    def copy_out(j):
        at = rows_of(j, 0, block)
        return pltpu.make_async_copy(new_ref.at[at, :], edge_out_ref.at[at, :], sems.at[j])

    def look(remote, b):
        marks = [marks_from(spread(remote, 2 * b + k), 2, 0) for k in range(2)]
        return dot(jnp.concatenate(marks, axis=0), tx)

    def hide(j, b, found):
        pre = pre_ref[rows_of(j, 2 * b * LANES, 2 * LANES), :] + found
        hidden_ref[2 * b * LANES : 2 * (b + 1) * LANES, :] = jnp.maximum(pre, 0.0).astype(BF16)

    def second(b):
        at = 2 * b * LANES
        top, bottom = hidden_ref[at : at + LANES, :], hidden_ref[at + LANES : at + 2 * LANES, :]
        return dot(jnp.concatenate([top, bottom], axis=1), w2) + b2

    def gather_part(j, b):
        at = slice(2 * b * LANES, 2 * (b + 1) * LANES)
        return dot(target_ref[:, rows_of(j, at.start, 2 * LANES)], packed_ref[at, :])

    def finish(j, b, centre, spreads, live, high):
        normed = centre * lax.rsqrt(spreads + EPSILON)
        for k in range(2):
            place = 2 * b + k
            at = rows_of(j, place * LANES, LANES)
            message = normed[:, k * LANES : (k + 1) * LANES] * gain + bias
            kept = message.astype(BF16) * spread(live, place)
            new_ref[at, :] = edge_ref[at, :] + kept
            upper = kept * spread(high, place)
            local = slice(place * LANES, (place + 1) * LANES)
            packed_ref[local, :LANES] = kept - upper
            packed_ref[local, LANES:] = upper

    def round_of(j, ahead, behind):
        live = tile_of(live_ref, j).astype(F32).T.astype(BF16)
        high = (tile_of(recv_ref, j) >= nodes_half).astype(F32).T.astype(BF16)
        if ahead:
            remote = (tile_of(send_ref, j + 1) - n).astype(F32).T.astype(BF16)
        centres, total, waiting = {}, None, []
        for b in range(quarters + 1):
            if b < quarters:
                centres[b] = second(b)
                if ahead:
                    found = look(remote, b)
            if b > 0:
                p = b - 1
                if behind:
                    part = gather_part(j - 1, p)
                    total = part if total is None else total + part
                spreads = dot((centres[p] * centres[p]).astype(BF16), averages)
                waiting.append((p, spreads))
            if b < quarters and ahead:
                hide(j + 1, b, found)
            if len(waiting) > 1 or b == quarters:
                for p, spreads in waiting[: len(waiting) if b == quarters else 1]:
                    finish(j, p, centres[p], spreads, live, high)
                waiting = waiting[1:]
        copy_out(j).start()
        if behind:
            acc_ref[...] += total

    steps = pre_ref.shape[0] // block
    remote = (tile_of(send_ref, 0) - n).astype(F32).T.astype(BF16)
    for b in range(quarters):
        hide(0, b, look(remote, b))
    round_of(0, True, False)

    for j in range(1, steps - 1):
        round_of(j, True, True)
    round_of(steps - 1, False, True)
    acc_ref[...] += dot(target_ref[:, rows_of(steps - 1, 0, block)], packed_ref[...])

    nb2 = nb2_ref[...]
    nb2 = nb2 - jnp.mean(nb2, axis=-1, keepdims=True)
    nb2 = jnp.concatenate([nb2, nb2], axis=1)
    nw2 = nw2_ref[...].astype(F32)
    nw2 = twice((nw2 - jnp.mean(nw2, axis=-1, keepdims=True)).astype(BF16))
    nw1, nb1 = nw1_ref[...], nb1_ref[...]
    parts = 4
    size = nodes_half // parts
    mine = lambda p, k: slice(k * nodes_half + p * size, k * nodes_half + (p + 1) * size)
    hidden = []
    for p in range(parts):
        both = []
        for k in range(2):
            inbound = acc_ref[p * size : (p + 1) * size, k * LANES : (k + 1) * LANES].astype(BF16)
            first = dot(jnp.concatenate([fresh_ref[mine(p, k), :], inbound], axis=1), nw1)
            both.append(jnp.maximum(first + nb1, 0.0).astype(BF16))
        hidden.append(jnp.concatenate(both, axis=1))
    centres = [dot(h, nw2) + nb2 for h in hidden]
    spreads = [dot((centre * centre).astype(BF16), averages) for centre in centres]
    node_copies = []
    for p in range(parts):
        normed = centres[p] * lax.rsqrt(spreads[p] + EPSILON)
        for k in range(2):
            update = normed[:, k * LANES : (k + 1) * LANES] * ngain_ref[...] + nbias_ref[...]
            at = mine(p, k)
            node_ref[at, :] = (fresh_ref[at, :].astype(F32) + update).astype(BF16)
            copy = pltpu.make_async_copy(
                node_ref.at[at, :], node_out_ref.at[at, :], node_sems.at[2 * p + k]
            )
            copy.start()
            node_copies.append(copy)
    for j in range(steps):
        copy_out(j).wait()
    for copy in node_copies:
        copy.wait()


def outward(near_partner, far, d):
    rows = far.shape[0] // 2
    even_pair = (d // 2) % 2 == 0
    plus = jnp.concatenate([far[rows:], near_partner[rows:]], axis=0)
    minus = jnp.concatenate([far[:rows], near_partner[:rows]], axis=0)
    outer = swapped(
        jnp.where(even_pair, minus, plus), "dom", lambda i: i - 2 if i % 4 < 2 else i + 2
    )
    inner = swapped(
        jnp.where(even_pair, plus, minus), "dom", lambda i: i + 2 if i % 4 < 2 else i - 2
    )
    return outer, inner


def inward(near_partner, outer, inner, d):
    rows = near_partner.shape[0] // 2
    odd = d % 2 == 1
    even_pair = (d // 2) % 2 == 0
    before = jnp.where(even_pair, outer, inner)
    after = jnp.where(even_pair, inner, outer)
    return jnp.concatenate(
        [
            after[:rows],
            jnp.where(odd, after[rows:], near_partner[:rows]),
            jnp.where(odd, near_partner[rows:], before[rows:]),
            before[:rows],
        ],
        axis=0,
    )


def call(kernel, out_shape, limit, flops=10**9, **kw):
    return pl.pallas_call(
        kernel,
        out_shape=out_shape,
        compiler_params=pltpu.CompilerParams(vmem_limit_bytes=limit << 20),
        cost_estimate=pl.CostEstimate(flops=flops, bytes_accessed=10**6, transcendentals=0),
        **kw,
    )


VM = pl.BlockSpec(memory_space=pltpu.VMEM)


def like(*arrays):
    return [jax.ShapeDtypeStruct(a.shape, a.dtype) for a in arrays]


def body(
    node_latent, edge_latent, mig_send, mig_recv, halo_send, cross_send, senders, receivers, edge_live,
    edge_w1, edge_b1, edge_w2, edge_b2, edge_gain, edge_bias,
    node_w1, node_b1, node_w2, node_b2, node_gain, node_bias,
):
    n, latent = node_latent.shape
    edges = edge_latent.shape[0]
    d = lax.axis_index("dom")
    move = mig_send.shape[1]
    halo = halo_send.shape[1]
    cross = cross_send.shape[1]
    shape = jax.ShapeDtypeStruct
    row = lambda v: v.reshape(1, latent)
    tiles = lambda v: v.reshape(-1, LANES)

    (first,) = call(first_kernel, [shape((8, LANES), F32)], 1)()
    near, far = call(
        leave_kernel, [shape((move // 2, latent), BF16)] * 2, 4, in_specs=[VM, VM, ANY]
    )(node_latent, mig_send, first)
    partner = swapped(near, "dom", lambda i: i ^ 1)
    args = (
        edge_latent, edge_w1, row(edge_b1), tiles(senders), tiles(receivers), tiles(edge_live),
        tiles(mig_recv), halo_send, cross_send,
    )
    own, w1, send, recv, live, mig, halo_index, cross_index = call(
        own_kernel,
        [shape((edges, latent), F32)] + like(args[1], *args[3:]),
        10,
        in_specs=[VM] * 9 + [ANY],
    )(*args, near)
    partner, own, recv = lax.optimization_barrier((partner, own, recv))
    outer, inner = outward(partner, far, d)
    (targets,) = call(
        target_kernel, [shape((n // 2, edges), BF16)], 10, in_specs=[VM, ANY]
    )(recv, partner)
    outer, inner, targets = lax.optimization_barrier((outer, inner, targets))
    arrived = inward(partner, outer, inner, d)

    fresh, near, far, cross_out = call(
        fresh_kernel,
        [shape((n, latent), BF16)] + [shape((halo // 2, latent), BF16)] * 2 + [shape((cross, latent), BF16)],
        8,
    )(node_latent, arrived, mig, halo_index, cross_index)
    partner = swapped(near, "dom", lambda i: i ^ 1)
    cross_in = lax.ppermute(cross_out, "grp", [(i, i ^ 1) for i in range(lax.axis_size("grp"))])
    (pre,) = call(
        functools.partial(pre_kernel, part=2), [shape((edges, latent), F32)], 10,
        in_specs=[VM] * 4 + [ANY],
    )(own, fresh, recv, w1, near)
    partner, pre = lax.optimization_barrier((partner, pre))
    outer, inner = outward(partner, far, d)
    (pre,) = call(
        functools.partial(pre_kernel, part=1), [shape((edges, latent), F32)], 10,
        in_specs=[VM] * 4 + [ANY],
    )(pre, fresh, send, w1, partner)
    outer, inner, cross_in, pre = lax.optimization_barrier((outer, inner, cross_in, pre))
    halo_in = inward(partner, outer, inner, d)
    node_out, edge_out = call(
        edge_kernel,
        [shape((n, latent), BF16), shape((edges, latent), BF16)],
        16,
        flops=10**10,
        out_specs=[ANY, ANY],
        scratch_shapes=[
            pltpu.VMEM((edges, latent), BF16),
            pltpu.VMEM((n // 2, 2 * latent), F32),
            pltpu.VMEM((EDGE_BLOCK, latent), BF16),
            pltpu.VMEM((EDGE_BLOCK, 2 * latent), BF16),
            pltpu.VMEM((n, latent), BF16),
            pltpu.SemaphoreType.DMA((edges // EDGE_BLOCK,)),
            pltpu.SemaphoreType.DMA((8,)),
        ],
    )(
        pre, edge_latent, fresh, halo_in, cross_in, send, recv, live, targets,
        w1, edge_w2, row(edge_b2), row(edge_gain), row(edge_bias),
        node_w1, row(node_b1), node_w2, row(node_b2), row(node_gain), row(node_bias),
    )
    return node_out, edge_out


def solution(mesh):
    split, split1, copied = P(("grp", "dom"), None), P(("grp", "dom")), P()
    placed = (
        split, split, split, split1, split, split, split1, split1, split1,
    ) + (copied,) * 12
    return jax.shard_map(
        body, mesh=mesh, in_specs=placed, out_specs=(split, split), check_vma=False
    )
```

```python
import functools

import jax
import jax.numpy as jnp
from jax import lax
from jax.experimental import pallas as pl
from jax.experimental.pallas import tpu as pltpu
from jax.sharding import PartitionSpec as P


LANES = 128
EDGE_BLOCK = 1024
ANY = pl.BlockSpec(memory_space=pl.ANY)
EPSILON = 1e-05
BF16 = jnp.bfloat16
F32 = jnp.float32


def dot(a, b):
    return jnp.dot(a, b, preferred_element_type=F32)


def swapped(value, axis, partner_of):
    count = lax.axis_size(axis)
    pairs = []
    for i in range(count):
        j = partner_of(i)
        pairs.append((i, j if 0 <= j < count else i ^ 1))
    return lax.ppermute(value, axis, pairs)


def lane_ids(tile, shift):
    ids = lax.broadcasted_iota(jnp.int32, (LANES, LANES), 1) + (tile * LANES - shift)
    return ids.astype(F32).astype(BF16)


def spread(columns, b):
    return jnp.broadcast_to(columns[:, b : b + 1], (columns.shape[0], LANES))


def marks_from(values, count, shift):
    one, zero = jnp.ones((), BF16), jnp.zeros((), BF16)
    rows = values.shape[0]
    return jnp.concatenate(
        [jnp.where(values == lane_ids(t, shift)[:rows], one, zero) for t in range(count)], axis=1
    )


def split_index(rows, half):
    high = (rows >= half).astype(F32)
    low = rows.astype(F32) - high * half - half // 2
    return low.T.astype(BF16), high.T


def lookup(low, high, b, table2):
    half = table2.shape[0]
    both = dot(marks_from(spread(low, b), half // LANES, half // 2), table2)
    return jnp.where(spread(high, b) > 0.5, both[:, LANES:], both[:, :LANES])


def side_by_side(table):
    half = table.shape[0] // 2
    return jnp.concatenate([table[:half], table[half:]], axis=1)


def twice(w):
    zero = jnp.zeros_like(w)
    return jnp.concatenate(
        [jnp.concatenate([w, zero], axis=1), jnp.concatenate([zero, w], axis=1)], axis=0
    )


def centred(w):
    return w - jnp.mean(w, axis=-1, keepdims=True)


def eight(row):
    return jnp.broadcast_to(row, (8, row.shape[1]))


def first_kernel(out_ref):
    out_ref[...] = jnp.zeros_like(out_ref)


def leave_kernel(node_ref, send_ref, _, near_ref, far_ref):
    table = side_by_side(node_ref[...])
    pieces = []
    for b in range(send_ref.shape[1] // LANES):
        low, high = split_index(eight(send_ref[:, b * LANES : (b + 1) * LANES]), table.shape[0])
        pieces.append(lookup(low, high, 0, table))
    rows = jnp.concatenate(pieces, axis=0).astype(BF16)
    quarter = rows.shape[0] // 4
    near_ref[...] = rows[quarter : 3 * quarter]
    far_ref[...] = jnp.concatenate([rows[:quarter], rows[3 * quarter :]], axis=0)


def own_kernel(
    edge_ref, w1_ref, b1_ref, send_ref, recv_ref, live_ref, mig_ref, halo_ref, cross_ref, _,
    own_ref, w1_copy, send_copy, recv_copy, live_copy, mig_copy, halo_copy, cross_copy,
):
    w1_copy[...] = w1_ref[...]
    send_copy[...] = send_ref[...]
    recv_copy[...] = recv_ref[...]
    live_copy[...] = live_ref[...]
    mig_copy[...] = mig_ref[...]
    halo_copy[...] = halo_ref[...]
    cross_copy[...] = cross_ref[...]
    wa = twice(w1_ref[:LANES, :])
    b1 = b1_ref[...]
    half = EDGE_BLOCK // 2

    def step(i, carry):
        at = pl.multiple_of(i * EDGE_BLOCK, EDGE_BLOCK)
        top, bottom = edge_ref[pl.ds(at, half), :], edge_ref[pl.ds(at + half, half), :]
        pair = dot(jnp.concatenate([top, bottom], axis=1), wa)
        own_ref[pl.ds(at, half), :] = pair[:, :LANES] + b1
        own_ref[pl.ds(at + half, half), :] = pair[:, LANES:] + b1
        return carry

    lax.fori_loop(0, edge_ref.shape[0] // EDGE_BLOCK, step, 0)


def target_marks(recv_ref, marks_ref):
    half = marks_ref.shape[1]
    one, zero = jnp.ones((), BF16), jnp.zeros((), BF16)
    ids = (lax.broadcasted_iota(jnp.int32, (half, LANES), 0) - half // 2).astype(F32).astype(BF16)
    recv = recv_ref[...]
    low = jnp.where(recv >= half, recv - half, recv) - half // 2
    low = low.astype(F32)
    for b in range(recv.shape[0]):
        row = jnp.broadcast_to(low[b : b + 1, :], (16, LANES)).astype(BF16)
        row = jnp.concatenate([row] * (half // 16), axis=0)
        at = b % 2 * LANES
        marks_ref[b // 2, :, at : at + LANES] = jnp.where(ids == row, one, zero)


def window_kernel(
    recv_ref, node_ref, mig_ref, _, marks_ref, old_ref, moved_ref,
):
    target_marks(recv_ref, marks_ref)
    table = side_by_side(node_ref[...])
    half_rows = table.shape[0]
    n = 2 * half_rows
    mig = mig_ref[...]
    low, high = split_index(mig, half_rows)
    moved = (mig - n).astype(F32).T.astype(BF16)
    count = moved_ref.shape[1] // LANES
    for b in range(n // LANES):
        at = slice(b * LANES, (b + 1) * LANES)
        old_ref[at, :] = lookup(low, high, b, table)
        moved_ref[at, :] = marks_from(spread(moved, b), count, 0)


def fresh_kernel(
    old_ref, moved_ref, halo_ref, cross_ref, arrived_ref, fresh_ref, near_ref, far_ref, cross_out
):
    fresh = (old_ref[...] + dot(moved_ref[...], arrived_ref[...])).astype(BF16)
    fresh_ref[...] = fresh
    table = side_by_side(fresh)
    low, high = split_index(eight(halo_ref[...]), table.shape[0])
    halo = lookup(low, high, 0, table).astype(BF16)
    quarter = halo.shape[0] // 4
    near_ref[...] = halo[quarter : 3 * quarter]
    far_ref[...] = jnp.concatenate([halo[:quarter], halo[3 * quarter :]], axis=0)
    low, high = split_index(eight(cross_ref[...]), table.shape[0])
    cross_out[...] = lookup(low, high, 0, table).astype(BF16)


def pre_kernel(before_ref, fresh_ref, index_ref, w_ref, _, out_ref, *, part):
    table = side_by_side(dot(fresh_ref[...], w_ref[part * LANES : (part + 1) * LANES, :]).astype(BF16))
    for i in range(out_ref.shape[0] // EDGE_BLOCK):
        low, high = split_index(index_ref[i * 8 : (i + 1) * 8, :], table.shape[0])
        for b in range(EDGE_BLOCK // LANES):
            at = slice(i * EDGE_BLOCK + b * LANES, i * EDGE_BLOCK + (b + 1) * LANES)
            out_ref[at, :] = before_ref[at, :] + lookup(low, high, b, table)


def edge_kernel(
    pre_ref, edge_ref, fresh_ref, halo_ref, cross_ref, send_ref, recv_ref, live_ref, target_ref,
    w1_ref, w2_ref, b2_ref, gain_ref, bias_ref,
    nw1_ref, nb1_ref, nw2_ref, nb2_ref, ngain_ref, nbias_ref,
    node_out_ref, edge_out_ref,
    new_ref, acc_ref, hidden_ref, packed_ref, node_ref, sems, node_sems,
):
    n = fresh_ref.shape[0]
    nodes_half = n // 2
    block = EDGE_BLOCK
    quarters = block // (2 * LANES)

    r = lax.broadcasted_iota(jnp.int32, (2 * LANES, 2 * LANES), 0) // LANES
    c = lax.broadcasted_iota(jnp.int32, (2 * LANES, 2 * LANES), 1) // LANES
    averages = jnp.where(r == c, 1.0 / LANES, 0.0).astype(BF16)
    b2 = b2_ref[...]
    b2 = b2 - jnp.mean(b2, axis=-1, keepdims=True)
    b2 = jnp.concatenate([b2, b2], axis=1)
    remote_rows = jnp.concatenate([halo_ref[...], cross_ref[...]], axis=0)
    tx = dot(remote_rows, w1_ref[LANES : 2 * LANES, :]).astype(BF16)
    tx = jnp.concatenate([tx, jnp.zeros((2 * LANES - tx.shape[0], LANES), BF16)], axis=0)
    w2 = twice(centred(w2_ref[...].astype(F32)).astype(BF16))
    gain, bias = gain_ref[...], bias_ref[...]
    acc_ref[...] = jnp.zeros_like(acc_ref)

    def rows_of(j, offset, size):
        return pl.ds(pl.multiple_of(j * block + offset, LANES), size)

    def tile_of(ref, j):
        return ref[pl.ds(pl.multiple_of(j * 8, 8), 8), :]

    def copy_out(j):
        at = rows_of(j, 0, block)
        return pltpu.make_async_copy(new_ref.at[at, :], edge_out_ref.at[at, :], sems.at[j])

    def look(remote, b):
        marks = [marks_from(spread(remote, 2 * b + k), 2, 0) for k in range(2)]
        return dot(jnp.concatenate(marks, axis=0), tx)

    def hide(j, b, found):
        pre = pre_ref[rows_of(j, 2 * b * LANES, 2 * LANES), :] + found
        hidden_ref[2 * b * LANES : 2 * (b + 1) * LANES, :] = jnp.maximum(pre, 0.0).astype(BF16)

    def second(b):
        at = 2 * b * LANES
        top, bottom = hidden_ref[at : at + LANES, :], hidden_ref[at + LANES : at + 2 * LANES, :]
        return dot(jnp.concatenate([top, bottom], axis=1), w2) + b2

    def gather_part(j, b):
        at = slice(2 * b * LANES, 2 * (b + 1) * LANES)
        return dot(target_ref[j * quarters + b], packed_ref[at, :])

    def finish(j, b, centre, spreads, live, high):
        normed = centre * lax.rsqrt(spreads + EPSILON)
        for k in range(2):
            place = 2 * b + k
            at = rows_of(j, place * LANES, LANES)
            message = normed[:, k * LANES : (k + 1) * LANES] * gain + bias
            kept = message.astype(BF16) * spread(live, place)
            new_ref[at, :] = edge_ref[at, :] + kept
            upper = kept * spread(high, place)
            local = slice(place * LANES, (place + 1) * LANES)
            packed_ref[local, :LANES] = kept - upper
            packed_ref[local, LANES:] = upper

    def round_of(j, ahead, behind):
        live = tile_of(live_ref, j).astype(F32).T.astype(BF16)
        high = (tile_of(recv_ref, j) >= nodes_half).astype(F32).T.astype(BF16)
        if ahead:
            remote = (tile_of(send_ref, j + 1) - n).astype(F32).T.astype(BF16)
        centres, total, waiting = {}, None, []
        for b in range(quarters + 1):
            if b < quarters:
                centres[b] = second(b)
                if ahead:
                    found = look(remote, b)
            if b > 0:
                p = b - 1
                if behind:
                    part = gather_part(j - 1, p)
                    total = part if total is None else total + part
                spreads = dot((centres[p] * centres[p]).astype(BF16), averages)
                waiting.append((p, spreads))
            if b < quarters and ahead:
                hide(j + 1, b, found)
            if len(waiting) > 1 or b == quarters:
                for p, spreads in waiting[: len(waiting) if b == quarters else 1]:
                    finish(j, p, centres[p], spreads, live, high)
                waiting = waiting[1:]
        copy_out(j).start()
        if behind:
            acc_ref[...] += total

    steps = pre_ref.shape[0] // block
    remote = (tile_of(send_ref, 0) - n).astype(F32).T.astype(BF16)
    for b in range(quarters):
        hide(0, b, look(remote, b))
    round_of(0, True, False)

    for j in range(1, steps - 1):
        round_of(j, True, True)
    round_of(steps - 1, False, True)
    acc_ref[...] += sum(gather_part(steps - 1, b) for b in range(quarters))

    nb2 = nb2_ref[...]
    nb2 = nb2 - jnp.mean(nb2, axis=-1, keepdims=True)
    nb2 = jnp.concatenate([nb2, nb2], axis=1)
    nw2 = twice(centred(nw2_ref[...].astype(F32)).astype(BF16))
    nw1, nb1 = nw1_ref[...], nb1_ref[...]
    parts = 4
    size = nodes_half // parts
    mine = lambda p, k: slice(k * nodes_half + p * size, k * nodes_half + (p + 1) * size)
    hidden = []
    for p in range(parts):
        both = []
        for k in range(2):
            inbound = acc_ref[p * size : (p + 1) * size, k * LANES : (k + 1) * LANES].astype(BF16)
            first = dot(jnp.concatenate([fresh_ref[mine(p, k), :], inbound], axis=1), nw1)
            both.append(jnp.maximum(first + nb1, 0.0).astype(BF16))
        hidden.append(jnp.concatenate(both, axis=1))
    centres = [dot(h, nw2) + nb2 for h in hidden]
    spreads = [dot((centre * centre).astype(BF16), averages) for centre in centres]
    node_copies = []
    for p in range(parts):
        normed = centres[p] * lax.rsqrt(spreads[p] + EPSILON)
        for k in range(2):
            update = normed[:, k * LANES : (k + 1) * LANES] * ngain_ref[...] + nbias_ref[...]
            at = mine(p, k)
            node_ref[at, :] = (fresh_ref[at, :].astype(F32) + update).astype(BF16)
            copy = pltpu.make_async_copy(
                node_ref.at[at, :], node_out_ref.at[at, :], node_sems.at[2 * p + k]
            )
            copy.start()
            node_copies.append(copy)
    for j in range(steps):
        copy_out(j).wait()
    for copy in node_copies:
        copy.wait()


def outward(near_partner, far, d):
    rows = far.shape[0] // 2
    even_pair = (d // 2) % 2 == 0
    plus = jnp.concatenate([far[rows:], near_partner[rows:]], axis=0)
    minus = jnp.concatenate([far[:rows], near_partner[:rows]], axis=0)
    outer = swapped(
        jnp.where(even_pair, minus, plus), "dom", lambda i: i - 2 if i % 4 < 2 else i + 2
    )
    inner = swapped(
        jnp.where(even_pair, plus, minus), "dom", lambda i: i + 2 if i % 4 < 2 else i - 2
    )
    return outer, inner


def inward(near_partner, outer, inner, d):
    rows = near_partner.shape[0] // 2
    odd = d % 2 == 1
    even_pair = (d // 2) % 2 == 0
    before = jnp.where(even_pair, outer, inner)
    after = jnp.where(even_pair, inner, outer)
    return jnp.concatenate(
        [
            after[:rows],
            jnp.where(odd, after[rows:], near_partner[:rows]),
            jnp.where(odd, near_partner[rows:], before[rows:]),
            before[:rows],
        ],
        axis=0,
    )


def call(kernel, out_shape, limit, flops=10**9, **kw):
    return pl.pallas_call(
        kernel,
        out_shape=out_shape,
        compiler_params=pltpu.CompilerParams(vmem_limit_bytes=limit << 20),
        cost_estimate=pl.CostEstimate(flops=flops, bytes_accessed=10**6, transcendentals=0),
        **kw,
    )


VM = pl.BlockSpec(memory_space=pltpu.VMEM)


def like(*arrays):
    return [jax.ShapeDtypeStruct(a.shape, a.dtype) for a in arrays]


def body(
    node_latent, edge_latent, mig_send, mig_recv, halo_send, cross_send, senders, receivers, edge_live,
    edge_w1, edge_b1, edge_w2, edge_b2, edge_gain, edge_bias,
    node_w1, node_b1, node_w2, node_b2, node_gain, node_bias,
):
    n, latent = node_latent.shape
    edges = edge_latent.shape[0]
    d = lax.axis_index("dom")
    move = mig_send.shape[1]
    halo = halo_send.shape[1]
    cross = cross_send.shape[1]
    shape = jax.ShapeDtypeStruct
    row = lambda v: v.reshape(1, latent)
    tiles = lambda v: v.reshape(-1, LANES)

    (first,) = call(first_kernel, [shape((8, LANES), F32)], 1)()
    near, far = call(
        leave_kernel, [shape((move // 2, latent), BF16)] * 2, 4, in_specs=[VM, VM, ANY]
    )(node_latent, mig_send, first)
    partner = swapped(near, "dom", lambda i: i ^ 1)
    args = (
        edge_latent, edge_w1, row(edge_b1), tiles(senders), tiles(receivers), tiles(edge_live),
        tiles(mig_recv), halo_send, cross_send,
    )
    own, w1, send, recv, live, mig, halo_index, cross_index = call(
        own_kernel,
        [shape((edges, latent), F32)] + like(args[1], *args[3:]),
        10,
        in_specs=[VM] * 9 + [ANY],
    )(*args, near)
    partner, own, recv = lax.optimization_barrier((partner, own, recv))
    outer, inner = outward(partner, far, d)
    targets, *late = call(
        window_kernel,
        [
            shape((edges // (2 * LANES), n // 2, 2 * LANES), BF16),
            shape((n, latent), F32), shape((n, move), BF16),
        ],
        12,
        in_specs=[VM] * 3 + [ANY],
    )(recv, node_latent, mig, partner)
    outer, inner, targets, *late = lax.optimization_barrier((outer, inner, targets, *late))
    arrived = inward(partner, outer, inner, d)

    fresh, near, far, cross_out = call(
        fresh_kernel,
        [shape((n, latent), BF16)] + [shape((halo // 2, latent), BF16)] * 2 + [shape((cross, latent), BF16)],
        8,
    )(*late, halo_index, cross_index, arrived)
    partner = swapped(near, "dom", lambda i: i ^ 1)
    cross_in = lax.ppermute(cross_out, "grp", [(i, i ^ 1) for i in range(lax.axis_size("grp"))])
    (pre,) = call(
        functools.partial(pre_kernel, part=2), [shape((edges, latent), F32)], 10,
        in_specs=[VM] * 4 + [ANY],
    )(own, fresh, recv, w1, near)
    partner, pre = lax.optimization_barrier((partner, pre))
    outer, inner = outward(partner, far, d)
    (pre,) = call(
        functools.partial(pre_kernel, part=1), [shape((edges, latent), F32)], 10,
        in_specs=[VM] * 4 + [ANY],
    )(pre, fresh, send, w1, partner)
    outer, inner, cross_in, pre = lax.optimization_barrier((outer, inner, cross_in, pre))
    halo_in = inward(partner, outer, inner, d)
    node_out, edge_out = call(
        edge_kernel,
        [shape((n, latent), BF16), shape((edges, latent), BF16)],
        16,
        flops=10**10,
        out_specs=[ANY, ANY],
        scratch_shapes=[
            pltpu.VMEM((edges, latent), BF16),
            pltpu.VMEM((n // 2, 2 * latent), F32),
            pltpu.VMEM((EDGE_BLOCK, latent), BF16),
            pltpu.VMEM((EDGE_BLOCK, 2 * latent), BF16),
            pltpu.VMEM((n, latent), BF16),
            pltpu.SemaphoreType.DMA((edges // EDGE_BLOCK,)),
            pltpu.SemaphoreType.DMA((8,)),
        ],
    )(
        pre, edge_latent, fresh, halo_in, cross_in, send, recv, live, targets,
        w1, edge_w2, row(edge_b2), row(edge_gain), row(edge_bias),
        node_w1, row(node_b1), node_w2, row(node_b2), row(node_gain), row(node_bias),
    )
    return node_out, edge_out


def solution(mesh):
    split, split1, copied = P(("grp", "dom"), None), P(("grp", "dom")), P()
    placed = (
        split, split, split, split1, split, split, split1, split1, split1,
    ) + (copied,) * 12
    return jax.shard_map(
        body, mesh=mesh, in_specs=placed, out_specs=(split, split), check_vma=False
    )
```

```python
import functools

import jax
import jax.numpy as jnp
from jax import lax
from jax.experimental import pallas as pl
from jax.experimental.pallas import tpu as pltpu
from jax.sharding import PartitionSpec as P


LANES = 128
EDGE_BLOCK = 1024
ANY = pl.BlockSpec(memory_space=pl.ANY)
EPSILON = 1e-05
BF16 = jnp.bfloat16
F32 = jnp.float32


def dot(a, b):
    return jnp.dot(a, b, preferred_element_type=F32)


def swapped(value, axis, partner_of):
    count = lax.axis_size(axis)
    pairs = []
    for i in range(count):
        j = partner_of(i)
        pairs.append((i, j if 0 <= j < count else i ^ 1))
    return lax.ppermute(value, axis, pairs)


def lane_ids(tile, shift):
    ids = lax.broadcasted_iota(jnp.int32, (LANES, LANES), 1) + (tile * LANES - shift)
    return ids.astype(F32).astype(BF16)


def spread(columns, b):
    return jnp.broadcast_to(columns[:, b : b + 1], (columns.shape[0], LANES))


def marks_from(values, count, shift):
    one, zero = jnp.ones((), BF16), jnp.zeros((), BF16)
    rows = values.shape[0]
    return jnp.concatenate(
        [jnp.where(values == lane_ids(t, shift)[:rows], one, zero) for t in range(count)], axis=1
    )


def split_index(rows, half):
    high = (rows >= half).astype(F32)
    low = rows.astype(F32) - high * half - half // 2
    return low.T.astype(BF16), high.T


def lookup(low, high, b, table2):
    half = table2.shape[0]
    both = dot(marks_from(spread(low, b), half // LANES, half // 2), table2)
    return jnp.where(spread(high, b) > 0.5, both[:, LANES:], both[:, :LANES])


def side_by_side(table):
    half = table.shape[0] // 2
    return jnp.concatenate([table[:half], table[half:]], axis=1)


def twice(w):
    zero = jnp.zeros_like(w)
    return jnp.concatenate(
        [jnp.concatenate([w, zero], axis=1), jnp.concatenate([zero, w], axis=1)], axis=0
    )


def centred(w):
    return w - jnp.mean(w, axis=-1, keepdims=True)


def eight(row):
    return jnp.broadcast_to(row, (8, row.shape[1]))


def first_kernel(out_ref):
    out_ref[...] = jnp.zeros_like(out_ref)


def leave_kernel(node_ref, send_ref, _, near_ref, far_ref):
    table = side_by_side(node_ref[...])
    pieces = []
    for b in range(send_ref.shape[1] // LANES):
        low, high = split_index(eight(send_ref[:, b * LANES : (b + 1) * LANES]), table.shape[0])
        pieces.append(lookup(low, high, 0, table))
    rows = jnp.concatenate(pieces, axis=0).astype(BF16)
    quarter = rows.shape[0] // 4
    near_ref[...] = rows[quarter : 3 * quarter]
    far_ref[...] = jnp.concatenate([rows[:quarter], rows[3 * quarter :]], axis=0)


def own_kernel(
    edge_ref, w1_ref, b1_ref, send_ref, recv_ref, live_ref, mig_ref, halo_ref, cross_ref, _,
    own_ref, w1_copy, send_copy, recv_copy, live_copy, mig_copy, halo_copy, cross_copy,
):
    w1_copy[...] = w1_ref[...]
    send_copy[...] = send_ref[...]
    recv_copy[...] = recv_ref[...]
    live_copy[...] = live_ref[...]
    mig_copy[...] = mig_ref[...]
    halo_copy[...] = halo_ref[...]
    cross_copy[...] = cross_ref[...]
    wa = twice(w1_ref[:LANES, :])
    b1 = b1_ref[...]
    half = EDGE_BLOCK // 2

    def step(i, carry):
        at = pl.multiple_of(i * EDGE_BLOCK, EDGE_BLOCK)
        top, bottom = edge_ref[pl.ds(at, half), :], edge_ref[pl.ds(at + half, half), :]
        pair = dot(jnp.concatenate([top, bottom], axis=1), wa)
        own_ref[pl.ds(at, half), :] = pair[:, :LANES] + b1
        own_ref[pl.ds(at + half, half), :] = pair[:, LANES:] + b1
        return carry

    lax.fori_loop(0, edge_ref.shape[0] // EDGE_BLOCK, step, 0)


def target_marks(recv_ref, marks_ref):
    half = marks_ref.shape[1]
    one, zero = jnp.ones((), BF16), jnp.zeros((), BF16)
    ids = (lax.broadcasted_iota(jnp.int32, (half, LANES), 0) - half // 2).astype(F32).astype(BF16)
    recv = recv_ref[...]
    low = jnp.where(recv >= half, recv - half, recv) - half // 2
    low = low.astype(F32)
    for b in range(recv.shape[0]):
        row = jnp.broadcast_to(low[b : b + 1, :], (16, LANES)).astype(BF16)
        row = jnp.concatenate([row] * (half // 16), axis=0)
        at = b % 2 * LANES
        marks_ref[b // 2, :, at : at + LANES] = jnp.where(ids == row, one, zero)


def window_kernel(
    recv_ref, node_ref, mig_ref, _, marks_ref, old_ref, moved_ref,
):
    target_marks(recv_ref, marks_ref)
    table = side_by_side(node_ref[...])
    half_rows = table.shape[0]
    n = 2 * half_rows
    mig = mig_ref[...]
    low, high = split_index(mig, half_rows)
    moved = (mig - n).astype(F32).T.astype(BF16)
    count = moved_ref.shape[1] // LANES
    for b in range(n // LANES):
        at = slice(b * LANES, (b + 1) * LANES)
        old_ref[at, :] = lookup(low, high, b, table).astype(BF16)
        moved_ref[at, :] = marks_from(spread(moved, b), count, 0)


def fresh_kernel(
    old_ref, moved_ref, halo_ref, cross_ref, arrived_ref, fresh_ref, near_ref, far_ref, cross_out
):
    fresh = (old_ref[...].astype(F32) + dot(moved_ref[...], arrived_ref[...])).astype(BF16)
    fresh_ref[...] = fresh
    table = side_by_side(fresh)
    low, high = split_index(eight(halo_ref[...]), table.shape[0])
    halo = lookup(low, high, 0, table).astype(BF16)
    quarter = halo.shape[0] // 4
    near_ref[...] = halo[quarter : 3 * quarter]
    far_ref[...] = jnp.concatenate([halo[:quarter], halo[3 * quarter :]], axis=0)
    low, high = split_index(eight(cross_ref[...]), table.shape[0])
    cross_out[...] = lookup(low, high, 0, table).astype(BF16)


def pre_kernel(before_ref, fresh_ref, index_ref, w_ref, _, out_ref, *, part):
    table = side_by_side(dot(fresh_ref[...], w_ref[part * LANES : (part + 1) * LANES, :]).astype(BF16))
    for i in range(out_ref.shape[0] // EDGE_BLOCK):
        low, high = split_index(index_ref[i * 8 : (i + 1) * 8, :], table.shape[0])
        for b in range(EDGE_BLOCK // LANES):
            at = slice(i * EDGE_BLOCK + b * LANES, i * EDGE_BLOCK + (b + 1) * LANES)
            out_ref[at, :] = before_ref[at, :] + lookup(low, high, b, table)


def edge_kernel(
    pre_ref, edge_ref, fresh_ref, halo_ref, cross_ref, send_ref, recv_ref, live_ref, target_ref,
    w1_ref, w2_ref, b2_ref, gain_ref, bias_ref,
    nw1_ref, nb1_ref, nw2_ref, nb2_ref, ngain_ref, nbias_ref,
    node_out_ref, edge_out_ref,
    new_ref, acc_ref, hidden_ref, packed_ref, node_ref, sems, node_sems,
):
    n = fresh_ref.shape[0]
    nodes_half = n // 2
    block = EDGE_BLOCK
    quarters = block // (2 * LANES)

    r = lax.broadcasted_iota(jnp.int32, (2 * LANES, 2 * LANES), 0) // LANES
    c = lax.broadcasted_iota(jnp.int32, (2 * LANES, 2 * LANES), 1) // LANES
    averages = jnp.where(r == c, 1.0 / LANES, 0.0).astype(BF16)
    b2 = b2_ref[...]
    b2 = b2 - jnp.mean(b2, axis=-1, keepdims=True)
    b2 = jnp.concatenate([b2, b2], axis=1)
    remote_rows = jnp.concatenate([halo_ref[...], cross_ref[...]], axis=0)
    tx = dot(remote_rows, w1_ref[LANES : 2 * LANES, :]).astype(BF16)
    tx = jnp.concatenate([tx, jnp.zeros((2 * LANES - tx.shape[0], LANES), BF16)], axis=0)
    w2 = twice(centred(w2_ref[...].astype(F32)).astype(BF16))
    gain, bias = gain_ref[...], bias_ref[...]
    acc_ref[...] = jnp.zeros_like(acc_ref)

    def rows_of(j, offset, size):
        return pl.ds(pl.multiple_of(j * block + offset, LANES), size)

    def tile_of(ref, j):
        return ref[pl.ds(pl.multiple_of(j * 8, 8), 8), :]

    def copy_out(j):
        at = rows_of(j, 0, block)
        return pltpu.make_async_copy(new_ref.at[at, :], edge_out_ref.at[at, :], sems.at[j])

    def look(remote, b):
        marks = [marks_from(spread(remote, 2 * b + k), 2, 0) for k in range(2)]
        return dot(jnp.concatenate(marks, axis=0), tx)

    def hide(j, b, found):
        pre = pre_ref[rows_of(j, 2 * b * LANES, 2 * LANES), :] + found
        hidden_ref[2 * b * LANES : 2 * (b + 1) * LANES, :] = jnp.maximum(pre, 0.0).astype(BF16)

    def second(b):
        at = 2 * b * LANES
        top, bottom = hidden_ref[at : at + LANES, :], hidden_ref[at + LANES : at + 2 * LANES, :]
        return dot(jnp.concatenate([top, bottom], axis=1), w2) + b2

    def gather_part(j, b):
        at = slice(2 * b * LANES, 2 * (b + 1) * LANES)
        return dot(target_ref[j * quarters + b], packed_ref[at, :])

    def finish(j, b, centre, spreads, live, high):
        normed = centre * lax.rsqrt(spreads + EPSILON)
        for k in range(2):
            place = 2 * b + k
            at = rows_of(j, place * LANES, LANES)
            message = normed[:, k * LANES : (k + 1) * LANES] * gain + bias
            kept = message.astype(BF16) * spread(live, place)
            new_ref[at, :] = edge_ref[at, :] + kept
            upper = kept * spread(high, place)
            local = slice(place * LANES, (place + 1) * LANES)
            packed_ref[local, :LANES] = kept - upper
            packed_ref[local, LANES:] = upper

    def round_of(j, ahead, behind):
        live = tile_of(live_ref, j).astype(F32).T.astype(BF16)
        high = (tile_of(recv_ref, j) >= nodes_half).astype(F32).T.astype(BF16)
        if ahead:
            remote = (tile_of(send_ref, j + 1) - n).astype(F32).T.astype(BF16)
        centres, total, waiting = {}, None, []
        for b in range(quarters + 1):
            if b < quarters:
                centres[b] = second(b)
                if ahead:
                    found = look(remote, b)
            if b > 0:
                p = b - 1
                if behind:
                    part = gather_part(j - 1, p)
                    total = part if total is None else total + part
                spreads = dot((centres[p] * centres[p]).astype(BF16), averages)
                waiting.append((p, spreads))
            if b < quarters and ahead:
                hide(j + 1, b, found)
            if len(waiting) > 1 or b == quarters:
                for p, spreads in waiting[: len(waiting) if b == quarters else 1]:
                    finish(j, p, centres[p], spreads, live, high)
                waiting = waiting[1:]
        copy_out(j).start()
        if behind:
            acc_ref[...] += total

    steps = pre_ref.shape[0] // block
    remote = (tile_of(send_ref, 0) - n).astype(F32).T.astype(BF16)
    for b in range(quarters):
        hide(0, b, look(remote, b))
    round_of(0, True, False)

    for j in range(1, steps - 1):
        round_of(j, True, True)
    round_of(steps - 1, False, True)
    acc_ref[...] += sum(gather_part(steps - 1, b) for b in range(quarters))

    nb2 = nb2_ref[...]
    nb2 = nb2 - jnp.mean(nb2, axis=-1, keepdims=True)
    nb2 = jnp.concatenate([nb2, nb2], axis=1)
    nw2 = twice(centred(nw2_ref[...].astype(F32)).astype(BF16))
    nw1, nb1 = nw1_ref[...], nb1_ref[...]
    parts = 4
    size = nodes_half // parts
    mine = lambda p, k: slice(k * nodes_half + p * size, k * nodes_half + (p + 1) * size)
    hidden = []
    for p in range(parts):
        both = []
        for k in range(2):
            inbound = acc_ref[p * size : (p + 1) * size, k * LANES : (k + 1) * LANES].astype(BF16)
            first = dot(jnp.concatenate([fresh_ref[mine(p, k), :], inbound], axis=1), nw1)
            both.append(jnp.maximum(first + nb1, 0.0).astype(BF16))
        hidden.append(jnp.concatenate(both, axis=1))
    centres = [dot(h, nw2) + nb2 for h in hidden]
    spreads = [dot((centre * centre).astype(BF16), averages) for centre in centres]
    node_copies = []
    for p in range(parts):
        normed = centres[p] * lax.rsqrt(spreads[p] + EPSILON)
        for k in range(2):
            update = normed[:, k * LANES : (k + 1) * LANES] * ngain_ref[...] + nbias_ref[...]
            at = mine(p, k)
            node_ref[at, :] = (fresh_ref[at, :].astype(F32) + update).astype(BF16)
            copy = pltpu.make_async_copy(
                node_ref.at[at, :], node_out_ref.at[at, :], node_sems.at[2 * p + k]
            )
            copy.start()
            node_copies.append(copy)
    for j in range(steps):
        copy_out(j).wait()
    for copy in node_copies:
        copy.wait()


def outward(near_partner, far, d):
    rows = far.shape[0] // 2
    even_pair = (d // 2) % 2 == 0
    plus = jnp.concatenate([far[rows:], near_partner[rows:]], axis=0)
    minus = jnp.concatenate([far[:rows], near_partner[:rows]], axis=0)
    outer = swapped(
        jnp.where(even_pair, minus, plus), "dom", lambda i: i - 2 if i % 4 < 2 else i + 2
    )
    inner = swapped(
        jnp.where(even_pair, plus, minus), "dom", lambda i: i + 2 if i % 4 < 2 else i - 2
    )
    return outer, inner


def inward(near_partner, outer, inner, d):
    rows = near_partner.shape[0] // 2
    odd = d % 2 == 1
    even_pair = (d // 2) % 2 == 0
    before = jnp.where(even_pair, outer, inner)
    after = jnp.where(even_pair, inner, outer)
    return jnp.concatenate(
        [
            after[:rows],
            jnp.where(odd, after[rows:], near_partner[:rows]),
            jnp.where(odd, near_partner[rows:], before[rows:]),
            before[:rows],
        ],
        axis=0,
    )


def call(kernel, out_shape, limit, flops=10**9, **kw):
    return pl.pallas_call(
        kernel,
        out_shape=out_shape,
        compiler_params=pltpu.CompilerParams(vmem_limit_bytes=limit << 20),
        cost_estimate=pl.CostEstimate(flops=flops, bytes_accessed=10**6, transcendentals=0),
        **kw,
    )


VM = pl.BlockSpec(memory_space=pltpu.VMEM)


def like(*arrays):
    return [jax.ShapeDtypeStruct(a.shape, a.dtype) for a in arrays]


def body(
    node_latent, edge_latent, mig_send, mig_recv, halo_send, cross_send, senders, receivers, edge_live,
    edge_w1, edge_b1, edge_w2, edge_b2, edge_gain, edge_bias,
    node_w1, node_b1, node_w2, node_b2, node_gain, node_bias,
):
    n, latent = node_latent.shape
    edges = edge_latent.shape[0]
    d = lax.axis_index("dom")
    move = mig_send.shape[1]
    halo = halo_send.shape[1]
    cross = cross_send.shape[1]
    shape = jax.ShapeDtypeStruct
    row = lambda v: v.reshape(1, latent)
    tiles = lambda v: v.reshape(-1, LANES)

    (first,) = call(first_kernel, [shape((8, LANES), F32)], 1)()
    near, far = call(
        leave_kernel, [shape((move // 2, latent), BF16)] * 2, 4, in_specs=[VM, VM, ANY]
    )(node_latent, mig_send, first)
    partner = swapped(near, "dom", lambda i: i ^ 1)
    args = (
        edge_latent, edge_w1, row(edge_b1), tiles(senders), tiles(receivers), tiles(edge_live),
        tiles(mig_recv), halo_send, cross_send,
    )
    own, w1, send, recv, live, mig, halo_index, cross_index = call(
        own_kernel,
        [shape((edges, latent), F32)] + like(args[1], *args[3:]),
        10,
        in_specs=[VM] * 9 + [ANY],
    )(*args, near)
    partner, own, recv = lax.optimization_barrier((partner, own, recv))
    outer, inner = outward(partner, far, d)
    targets, *late = call(
        window_kernel,
        [
            shape((edges // (2 * LANES), n // 2, 2 * LANES), BF16),
            shape((n, latent), BF16), shape((n, move), BF16),
        ],
        12,
        in_specs=[VM] * 3 + [ANY],
    )(recv, node_latent, mig, partner)
    outer, inner, targets, *late = lax.optimization_barrier((outer, inner, targets, *late))
    arrived = inward(partner, outer, inner, d)

    fresh, near, far, cross_out = call(
        fresh_kernel,
        [shape((n, latent), BF16)] + [shape((halo // 2, latent), BF16)] * 2 + [shape((cross, latent), BF16)],
        8,
    )(*late, halo_index, cross_index, arrived)
    partner = swapped(near, "dom", lambda i: i ^ 1)
    cross_in = lax.ppermute(cross_out, "grp", [(i, i ^ 1) for i in range(lax.axis_size("grp"))])
    (pre,) = call(
        functools.partial(pre_kernel, part=2), [shape((edges, latent), F32)], 10,
        in_specs=[VM] * 4 + [ANY],
    )(own, fresh, recv, w1, near)
    partner, pre = lax.optimization_barrier((partner, pre))
    outer, inner = outward(partner, far, d)
    (pre,) = call(
        functools.partial(pre_kernel, part=1), [shape((edges, latent), F32)], 10,
        in_specs=[VM] * 4 + [ANY],
    )(pre, fresh, send, w1, partner)
    outer, inner, cross_in, pre = lax.optimization_barrier((outer, inner, cross_in, pre))
    halo_in = inward(partner, outer, inner, d)
    node_out, edge_out = call(
        edge_kernel,
        [shape((n, latent), BF16), shape((edges, latent), BF16)],
        16,
        flops=10**10,
        out_specs=[ANY, ANY],
        scratch_shapes=[
            pltpu.VMEM((edges, latent), BF16),
            pltpu.VMEM((n // 2, 2 * latent), F32),
            pltpu.VMEM((EDGE_BLOCK, latent), BF16),
            pltpu.VMEM((EDGE_BLOCK, 2 * latent), BF16),
            pltpu.VMEM((n, latent), BF16),
            pltpu.SemaphoreType.DMA((edges // EDGE_BLOCK,)),
            pltpu.SemaphoreType.DMA((8,)),
        ],
    )(
        pre, edge_latent, fresh, halo_in, cross_in, send, recv, live, targets,
        w1, edge_w2, row(edge_b2), row(edge_gain), row(edge_bias),
        node_w1, row(node_b1), node_w2, row(node_b2), row(node_gain), row(node_bias),
    )
    return node_out, edge_out


def solution(mesh):
    split, split1, copied = P(("grp", "dom"), None), P(("grp", "dom")), P()
    placed = (
        split, split, split, split1, split, split, split1, split1, split1,
    ) + (copied,) * 12
    return jax.shard_map(
        body, mesh=mesh, in_specs=placed, out_specs=(split, split), check_vma=False
    )
```
